32 devices in a mesh: groups: 2 (over x), req: 16 (over z, y, core).
Axes of the slice: x: 2, y: 2, z: 4, core: 2. Of those that a mesh axis runs over, the one named last changes fastest.
Arguments:
- cache_states: bfloat16 [32, 16, 8192], P(('groups', 'req')), parts along dimension 0, may hold values from -6 to 6
- pool_keys: bfloat16 [512, 64, 512], P(('groups', 'req')), parts along dimension 0, may hold values from -64 to 64
- pool_values: bfloat16 [512, 64, 512], P(('groups', 'req')), parts along dimension 0, may hold values from -6 to 6
- slot_prefix: int32 [32], P('groups'), parts along dimension 0, may hold values from 0 to 15, each once
- page_table: int32 [32, 16], P('groups'), parts along dimension 0, may hold values from 0 to 15, each once within a row
- prefix_id: int32 [32], P('groups'), parts along dimension 0, may hold values from 0 to 15
- lengths: int32 [32], P(('groups', 'req')), parts along dimension 0, may hold values from 32 to 128, as said below
- queries: bfloat16 [4096, 4096], P(('groups', 'req')), parts along dimension 0, may hold values from -64 to 64
- suffix_keys: bfloat16 [4096, 512], P(('groups', 'req')), parts along dimension 0, may hold values from -6 to 6
- suffix_values: bfloat16 [4096, 512], P(('groups', 'req')), parts along dimension 0, may hold values from -6 to 6
- u_in: bfloat16 [4096, 8192], P(('groups', 'req')), parts along dimension 0, may hold values from -6 to 6
- dt_raw: bfloat16 [4096, 8192], P(('groups', 'req')), parts along dimension 0, may hold values from -3 to 3
- bc_in: float32 [32, 32, 128], P(('groups', 'req')), parts along dimension 0, may hold values from -6 to 6
- a_log: float32 [16, 8192], replicated, may hold values from 0 to 2.77
- dt_bias: float32 [8192], replicated, may hold values from -7 to -2.3
- d_skip: float32 [8192], replicated, may hold values from 0.5 to 1.5
Outputs:
- mamba_out: bfloat16 [4096, 8192], P(('groups', 'req')), parts along dimension 0
- attn_out: bfloat16 [4096, 4096], P(('groups', 'req')), parts along dimension 0
- final_state: float32 [32, 16, 8192], P(('groups', 'req')), parts along dimension 0
The draws below stay inside these ranges and needn't reach their ends.
There are 2 independent parts, one for each index of `groups`. The reference program is written for one: setup_inputs(seed, part) draws one part's arguments, and reference() takes and returns one part's arrays. A program takes and returns all parts, laid end to end along the dimension named above; an argument that names none is the same for every part. Nothing has to cross between parts.
Inputs may be any that keep to these rules, and one draw needn't show every extreme that they name: `slot_prefix`: each prefix is held by exactly one slot. `page_table`: each row is a permutation of the local pages. `lengths`: some request has exactly 128 live tokens.
All inputs are finite; a program needn't handle non-finite values.
Results may differ from the reference program's by a relative error of at most 0.0049.
Values may be sent and summed in bfloat16 or wider, within the bound.
A program may use at most 128 MiB of HBM per device.

```python
import math
import jax
import jax.numpy as jnp
import numpy as np
from jax import lax

DW = 8192
NSTATE = 16
QH = 32
KH = 4
HD = 128
PAGE = 64
L = 128
PAGES = 16
REQS = 16
NPRE = 16


def draw_queries(key, part):
    shape = (REQS * L, QH * HD)
    base = jax.random.truncated_normal(jax.random.fold_in(key, 12), -6.0, 6.0, shape, jnp.float32)
    return base.astype(jnp.bfloat16)


def draw_pool_keys(key, part):
    shape = (NPRE * PAGES, PAGE, KH * HD)
    base = jax.random.truncated_normal(jax.random.fold_in(key, 14), -6.0, 6.0, shape, jnp.float32)
    return base.astype(jnp.bfloat16)


def draw_lengths(key, part):
    counts = jax.random.randint(jax.random.fold_in(key, 21), (REQS,), L // 4, L + 1, jnp.int32)
    chosen = jax.random.randint(jax.random.fold_in(key, 22), (), 0, REQS, jnp.int32)
    return counts.at[chosen].set(L)


def plant(values, key, low, largest):
    shape = values.shape
    index_at = [jax.random.randint(jax.random.fold_in(key, axis), (), 0, shape[axis]) for axis in range(len(shape))]
    values = values.at[tuple(index_at)].set(low)
    longest = shape.index(max(shape))
    index_at[longest] = (index_at[longest] + 1) % shape[longest]
    return values.at[tuple(index_at)].set(largest)


def block_levels(key, extent, cuts, smallest, top_value):
    level, own = 1.0, jax.random.fold_in(key, 6)
    for dim, shards_of in cuts:
        steps = jnp.exp(jax.random.uniform(jax.random.fold_in(own, dim), (shards_of,), jnp.float32, smallest / len(cuts), top_value / len(cuts)))
        level = level * jnp.repeat(steps, extent[dim] // shards_of).reshape([-1 if axis == dim else 1 for axis in range(len(extent))])
    return level


def cumulative_ranks(number_of, slope):
    portions = [(1 << 20) // math.isqrt(standing ** slope) + 1 for standing in range(1, number_of + 1)]
    spread = 1 + sum(portions) // (1 << 30)
    return np.cumsum(np.array([max(1, weight // spread) for weight in portions]))


def skewed_ids(rng, extent, amount, skew):
    table = cumulative_ranks(amount, skew)
    pick = jax.random.randint(jax.random.fold_in(rng, 1), extent, 0, int(table[amount - 1]))
    rank = jnp.searchsorted(jnp.asarray(table, jnp.int32), pick, side="right")
    return jax.random.permutation(jax.random.fold_in(rng, 2), amount)[rank].astype(jnp.int32)


def gaussian(rng, shape, deviation, bound, cuts=(), kind=jnp.bfloat16):
    drawn = jax.random.normal(rng, shape, jnp.float32) * deviation
    if len(cuts) > 0:
        drawn = block_levels(rng, shape, cuts, -0.22, 0.18) * drawn
    return jnp.clip(drawn, min=-bound, max=bound).astype(kind)


def setup_inputs(seed: int = 0, part: int = 0) -> dict:
    keys = jax.random.split(jax.random.key(seed), 17)
    part_splits = jax.random.split(jax.random.fold_in(keys[16], part), 17)
    cache_states = gaussian(part_splits[0], (NPRE, NSTATE, DW), 1.0, 6.0, ((0, 16),))
    pool_keys = draw_pool_keys(jax.random.fold_in(jax.random.fold_in(keys[16], part), 71), part)
    pool_values = gaussian(part_splits[2], (NPRE * PAGES, PAGE, KH * HD), 1.0, 6.0, ((0, 16),))
    slot_prefix = jax.random.permutation(part_splits[3], NPRE).astype(jnp.int32)
    page_table = jax.vmap(lambda own: jax.random.permutation(own, PAGES))(jax.random.split(part_splits[4], NPRE)).reshape((NPRE, PAGES)).astype(jnp.int32)
    prefix_id = plant(skewed_ids(part_splits[5], (REQS,), NPRE, 2), jax.random.fold_in(part_splits[5], 3), 0, NPRE - 1).astype(jnp.int32)
    lengths = draw_lengths(jax.random.fold_in(jax.random.fold_in(keys[16], part), 71), part)
    queries = draw_queries(jax.random.fold_in(jax.random.fold_in(keys[16], part), 71), part)
    suffix_keys = gaussian(part_splits[8], (REQS * L, KH * HD), 1.0, 6.0, ((0, 16),))
    suffix_values = gaussian(part_splits[9], (REQS * L, KH * HD), 1.0, 6.0, ((0, 16),))
    u_in = gaussian(part_splits[10], (REQS * L, DW), 1.0, 6.0, ((0, 16),))
    dt_raw = gaussian(part_splits[11], (REQS * L, DW), 0.5, 3.0, ((0, 16),))
    bc_in = gaussian(part_splits[12], (REQS, 2 * NSTATE, L), 1.0, 6.0, ((0, 16),), jnp.float32)
    a_log = jnp.clip(jax.random.uniform(keys[13], (NSTATE, DW), jnp.float32, 0.0, 2.77), 0.0, 2.77)
    dt_bias = jnp.clip(jax.random.uniform(keys[14], (DW,), jnp.float32, -7.0, -2.3), -7.0, -2.3)
    d_skip = jnp.clip(jax.random.uniform(keys[15], (DW,), jnp.float32, 0.5, 1.5), 0.5, 1.5)
    return {"cache_states": cache_states, "pool_keys": pool_keys, "pool_values": pool_values, "slot_prefix": slot_prefix, "page_table": page_table, "prefix_id": prefix_id, "lengths": lengths, "queries": queries, "suffix_keys": suffix_keys, "suffix_values": suffix_values, "u_in": u_in, "dt_raw": dt_raw, "bc_in": bc_in, "a_log": a_log, "dt_bias": dt_bias, "d_skip": d_skip}


def scan_tokens(start_state, u_rows, dt_rows, bc_rows, a_log, dt_bias, d_skip, length):
    rates = -jnp.exp(a_log)
    position = jnp.arange(u_rows.shape[0], dtype=jnp.int32)
    live_rows = (position < length).astype(jnp.float32)[:, None]
    deltas = jax.nn.softplus(dt_rows.astype(jnp.float32) + dt_bias[None, :]) * live_rows
    inputs = u_rows.astype(jnp.float32)

    def advance(carried, sliced):
        delta_row, input_row, b_col, c_col = sliced
        carried = jnp.exp(delta_row[None, :] * rates) * carried + (delta_row * input_row)[None, :] * b_col[:, None]
        return (carried, lax.optimization_barrier(jnp.sum(c_col[:, None] * carried, axis=0)))
    last_state, scanned = lax.scan(advance, start_state, (deltas, inputs, jnp.transpose(bc_rows[:NSTATE]), jnp.transpose(bc_rows[NSTATE:])))
    outputs = scanned + d_skip[None, :] * inputs
    return ((outputs * live_rows).astype(jnp.bfloat16), last_state)

def attend(query_rows, prefix_keys, prefix_values, suffix_keys, suffix_values, length):
    row_count = query_rows.shape[0]
    q_group = QH // KH
    prefix_len = prefix_keys.shape[0]
    keys_all = jnp.concatenate([prefix_keys, suffix_keys], axis=0)
    values_all = jnp.concatenate([prefix_values, suffix_values], axis=0)
    position = jnp.arange(row_count, dtype=jnp.int32)
    key_pos = jnp.arange(prefix_len + row_count, dtype=jnp.int32) - prefix_len
    visible = (key_pos[None, :] <= position[:, None]) & (key_pos[None, :] > position[:, None] - prefix_len)
    score_scale = 1.0 / math.sqrt(HD)
    pieces = []
    for kv_head in range(KH):
        q_block = query_rows[:, kv_head * q_group * HD:(kv_head + 1) * q_group * HD].reshape(row_count * q_group, HD)
        k_block = keys_all[:, kv_head * HD:(kv_head + 1) * HD]
        scores = lax.dot_general(q_block, k_block, (((1,), (1,)), ((), ())), preferred_element_type=jnp.float32) * score_scale
        scores = scores.reshape(row_count, q_group, -1)
        scores = jnp.where(visible[:, None, :], scores, -1e+30)
        highest = lax.optimization_barrier(jnp.max(scores, axis=2, keepdims=True))
        exponent = jnp.exp(scores - highest)
        totals = lax.optimization_barrier(jnp.sum(exponent, axis=2, keepdims=True))
        weights = (exponent / totals).astype(jnp.bfloat16).reshape(row_count * q_group, -1)
        mixed_rows = jnp.dot(weights, values_all[:, kv_head * HD:(kv_head + 1) * HD], preferred_element_type=jnp.float32)
        pieces.append(mixed_rows.astype(jnp.bfloat16).reshape(row_count, q_group * HD))
    result = jnp.concatenate(pieces, axis=1)
    live_rows = (position < length)[:, None]
    return jnp.where(live_rows, result, jnp.zeros_like(result))

def reference(cache_states, pool_keys, pool_values, slot_prefix, page_table, prefix_id, lengths, queries, suffix_keys, suffix_values, u_in, dt_raw, bc_in, a_log, dt_bias, d_skip):
    slot_count = slot_prefix.shape[0]
    page_count = page_table.shape[1]
    matches = (slot_prefix[None, :] == prefix_id[:, None]).astype(jnp.int32)
    source = lax.optimization_barrier(jnp.sum(matches * jnp.arange(slot_count, dtype=jnp.int32)[None, :], axis=1)).astype(jnp.int32)

    def one_request(request):
        owner_slot = source[request]
        prefix = prefix_id[request]
        pool_rows = (owner_slot * page_count + page_table[prefix]).astype(jnp.int32)
        prefix_keys = jnp.take(pool_keys, pool_rows, axis=0).reshape(-1, KH * HD)
        prefix_values = jnp.take(pool_values, pool_rows, axis=0).reshape(-1, KH * HD)
        start_state = cache_states[owner_slot].astype(jnp.float32)
        first_row = (request * L).astype(jnp.int32)
        query_rows = lax.dynamic_slice_in_dim(queries, first_row, L, 0)
        key_rows = lax.dynamic_slice_in_dim(suffix_keys, first_row, L, 0)
        value_rows = lax.dynamic_slice_in_dim(suffix_values, first_row, L, 0)
        u_rows = lax.dynamic_slice_in_dim(u_in, first_row, L, 0)
        dt_rows = lax.dynamic_slice_in_dim(dt_raw, first_row, L, 0)
        length = lengths[request]
        mamba_rows, last_state = scan_tokens(start_state, u_rows, dt_rows, bc_in[request], a_log, dt_bias, d_skip, length)
        attn_rows = attend(query_rows, prefix_keys, prefix_values, key_rows, value_rows, length)
        return (mamba_rows, attn_rows, last_state)
    mamba_all, attn_all, states = lax.map(one_request, jnp.arange(REQS, dtype=jnp.int32))
    return (mamba_all.reshape(REQS * L, DW), attn_all.reshape(REQS * L, QH * HD), states)
```

```python
import functools
import math

import jax
import jax.numpy as jnp
from jax import lax
from jax.experimental import pallas as pl
from jax.experimental.pallas import tpu as pltpu
from jax.sharding import PartitionSpec as P

HD = 128
MESH = pl.DeviceIdType.MESH
LOG2E = 1.4426950408889634
SUB = 8
LANE = 128
WIDE = SUB * LANE


def kernel(
    n,
    source,
    chunk_order,
    lengths,
    bc_cols,
    dt_bias,
    d_skip,
    cache,
    pool_k,
    pool_v,
    q_hbm,
    sk_hbm,
    sv_hbm,
    u_hbm,
    dt_hbm,
    a_hbm,
    mamba_hbm,
    attn_hbm,
    final_hbm,
    held_s,
    held_k,
    held_v,
    send_s,
    send_k,
    send_v,
    got_s,
    got_k,
    got_v,
    keys,
    values,
    q_v,
    u_v,
    dt_v,
    a_v,
    mamba_v,
    attn_v,
    final_v,
    delta_w,
    du_w,
    y_w,
    h_w,
    rate_w,
    bc_w,
    w_w,
    inv_w,
    send_sem,
    recv_sem,
    own_sem,
    in_sem,
    out_sem,
):
    me = lax.axis_index("req")
    tokens, channels = u_v.shape
    nstate = a_v.shape[0]
    blocks = channels // WIDE
    width = held_s.shape[2]
    total = keys.shape[0]
    prefix_len = total - tokens
    chunks, size, _ = got_k.shape
    per = chunks // n
    heads = q_v.shape[1] // HD
    q_group = heads // (keys.shape[1] // HD)

    loads = [
        pltpu.make_async_copy(dt_hbm, dt_v, in_sem.at[0]),
        pltpu.make_async_copy(u_hbm, u_v, in_sem.at[1]),
        pltpu.make_async_copy(a_hbm, a_v, in_sem.at[2]),
        pltpu.make_async_copy(q_hbm, q_v, in_sem.at[3]),
        pltpu.make_async_copy(sk_hbm, keys.at[pl.ds(prefix_len, tokens)], in_sem.at[4]),
        pltpu.make_async_copy(sv_hbm, values.at[pl.ds(prefix_len, tokens)], in_sem.at[5]),
    ]
    for load in loads:
        load.start()

    barrier = pltpu.get_barrier_semaphore()

    def greet(d, c):
        peer = lax.rem(me + d, n)
        pl.semaphore_signal(barrier, inc=1, device_id={"req": peer}, device_id_type=MESH)
        return c

    lax.fori_loop(1, n, greet, 0)
    pl.semaphore_wait(barrier, n - 1)

    def part(kind, index):
        if kind == 0:
            return cache.at[:, pl.ds(pl.multiple_of(index * width, width), width)]
        pool = pool_k if kind == 1 else pool_v
        return pool.at[pl.ds(index * per, per)]

    held = (held_s, held_k, held_v)
    outgoing = (send_s, send_k, send_v)
    got = (got_s, got_k, got_v)

    def spread(kind):
        own = pltpu.make_async_copy(part(kind, me), held[kind].at[me], own_sem.at[kind])
        own.start()

        def step(d, c):
            peer = lax.rem(me + d, n)
            pltpu.make_async_remote_copy(
                src_ref=part(kind, peer),
                dst_ref=held[kind].at[me],
                send_sem=send_sem.at[kind],
                recv_sem=recv_sem.at[kind],
                device_id={"req": peer},
                device_id_type=MESH,
            ).start()
            return c

        lax.fori_loop(1, n, step, 0)

    def settle(ref, sem):
        piece = ref.at[pl.ds(0, ref.shape[0] // n * (n - 1))]
        pltpu.make_async_copy(piece, piece, sem).wait()

    def collect(kind):
        settle(held[kind], recv_sem.at[kind])
        pltpu.make_async_copy(part(kind, me), held[kind].at[me], own_sem.at[kind]).wait()

        def pick(r, c):
            outgoing[kind][r] = held[kind][source[r]]
            return c

        lax.fori_loop(0, n, pick, 0)
        landing = got_s.at[me] if kind == 0 else got[kind].at[pl.ds(me * per, per)]
        if kind == 0:
            got_s[me] = held_s[source[me]]
        else:
            got[kind][pl.ds(me * per, per)] = held[kind][source[me]]

        def step(d, c):
            peer = lax.rem(me + d, n)
            pltpu.make_async_remote_copy(
                src_ref=outgoing[kind].at[peer],
                dst_ref=landing,
                send_sem=send_sem.at[3 + kind],
                recv_sem=recv_sem.at[3 + kind],
                device_id={"req": peer},
                device_id_type=MESH,
            ).start()
            return c

        lax.fori_loop(1, n, step, 0)

    spread(0)
    spread(1)

    def widen(k, c):
        column = jnp.broadcast_to(bc_cols[k], (tokens, LANE))
        for s in range(SUB):
            bc_w[k, pl.ds(s, tokens, stride=SUB), :] = column
        return c

    lax.fori_loop(0, 2 * nstate, widen, 0)

    length = lengths[0]
    live = lax.broadcasted_iota(jnp.int32, (tokens, LANE), 0) < length
    loads[0].wait()
    loads[1].wait()

    def steps_of(b, c):
        for s in range(SUB):
            at = pl.ds(pl.multiple_of(b * WIDE + s * LANE, LANE), LANE)
            raw = dt_v[:, at].astype(jnp.float32) + dt_bias[:, at]
            soft = jnp.maximum(raw, 0.0) + jnp.log1p(jnp.exp(-jnp.abs(raw)))
            delta = jnp.where(live, soft, 0.0)
            delta_w[b, pl.ds(s, tokens, stride=SUB), :] = delta
            du_w[b, pl.ds(s, tokens, stride=SUB), :] = delta * u_v[:, at].astype(jnp.float32)
        return c

    lax.fori_loop(0, blocks, steps_of, 0)
    collect(0)
    spread(2)
    loads[2].wait()

    def rates_of(b, c):
        for s in range(SUB):
            at = pl.ds(pl.multiple_of(b * WIDE + s * LANE, LANE), LANE)
            rate_w[b, pl.ds(s, nstate, stride=SUB), :] = -LOG2E * jnp.exp(a_v[:, at])
        return c

    lax.fori_loop(0, blocks, rates_of, 0)
    collect(1)
    settle(got_s, recv_sem.at[3])

    def scan_block(b, c):
        for s in range(SUB):
            first = b * WIDE + s * LANE
            inside = lax.rem(first, width)
            start = got_s[lax.div(first, width), :, pl.ds(pl.multiple_of(inside, LANE), LANE)]
            h_w[pl.ds(s, nstate, stride=SUB), :] = start.astype(jnp.float32)
        rates = [rate_w[b, pl.ds(k * SUB, SUB), :] for k in range(nstate)]

        def advance(t, hs):
            at = pl.ds(pl.multiple_of(t * SUB, SUB), SUB)
            delta = delta_w[b, at, :]
            du = du_w[b, at, :]
            new = []
            sums = [None, None]
            for k in range(nstate):
                h = jnp.exp2(delta * rates[k]) * hs[k] + du * bc_w[k, at, :]
                term = bc_w[nstate + k, at, :] * h
                sums[k % 2] = term if sums[k % 2] is None else sums[k % 2] + term
                new.append(h)
            y_w[at, :] = sums[0] + sums[1]
            return tuple(new)

        def pair(i, hs):
            return advance(2 * i + 1, advance(2 * i, hs))

        hs = tuple(h_w[pl.ds(k * SUB, SUB), :] for k in range(nstate))
        hs = lax.fori_loop(0, tokens // 2, pair, hs)
        for k in range(nstate):
            h_w[pl.ds(k * SUB, SUB), :] = hs[k]
        for s in range(SUB):
            at = pl.ds(pl.multiple_of(b * WIDE + s * LANE, LANE), LANE)
            final_v[:, at] = h_w[pl.ds(s, nstate, stride=SUB), :]
            y = y_w[pl.ds(s, tokens, stride=SUB), :] + d_skip[:, at] * u_v[:, at].astype(jnp.float32)
            mamba_v[:, at] = jnp.where(live, y, 0.0).astype(jnp.bfloat16)
        return c

    half = blocks // 2
    lax.fori_loop(0, half, scan_block, 0)
    collect(2)
    lax.fori_loop(half, blocks, scan_block, 0)

    stores = [
        pltpu.make_async_copy(mamba_v, mamba_hbm, out_sem.at[0]),
        pltpu.make_async_copy(final_v, final_hbm, out_sem.at[1]),
        pltpu.make_async_copy(attn_v, attn_hbm, out_sem.at[2]),
    ]
    stores[0].start()
    stores[1].start()

    def order(kind, into):
        def step(k, c):
            to = pl.ds(pl.multiple_of(k * size, size), size)
            into[to, :] = got[kind][chunk_order[k]]
            return c

        lax.fori_loop(0, chunks, step, 0)

    loads[3].wait()
    loads[4].wait()
    settle(got_k, recv_sem.at[4])
    order(1, keys)
    factor = LOG2E / math.sqrt(HD)
    row = lax.broadcasted_iota(jnp.int32, (tokens, tokens), 0)
    col = lax.broadcasted_iota(jnp.int32, (tokens, tokens), 1)

    def weigh(j):
        g = lax.div(j, q_group)
        q = q_v[:, pl.ds(pl.multiple_of(j * HD, HD), HD)]
        k = keys[:, pl.ds(pl.multiple_of(g * HD, HD), HD)]
        scores = lax.dot_general(q, k, (((1,), (1,)), ((), ())), preferred_element_type=jnp.float32)
        scores = jnp.concatenate(
            [
                jnp.where(col > row, scores[:, :tokens], -1e30),
                scores[:, tokens:prefix_len],
                jnp.where(col <= row, scores[:, prefix_len:], -1e30),
            ],
            axis=1,
        )
        highest = jnp.max(scores, axis=1, keepdims=True)
        weight = jnp.exp2((scores - highest) * factor)
        inv_w[j] = jnp.broadcast_to(1.0 / jnp.sum(weight, axis=1, keepdims=True), (tokens, HD))
        w_w[j] = weight.astype(jnp.bfloat16)

    def weigh_pair(i, c):
        weigh(2 * i)
        weigh(2 * i + 1)
        return c

    lax.fori_loop(0, heads // 2, weigh_pair, 0)

    loads[5].wait()
    settle(got_v, recv_sem.at[5])
    order(2, values)

    def mix(j):
        g = lax.div(j, q_group)
        v = values[:, pl.ds(pl.multiple_of(g * HD, HD), HD)]
        out = jnp.dot(w_w[j], v, preferred_element_type=jnp.float32) * inv_w[j]
        out = jnp.where(live, out, 0.0)
        attn_v[:, pl.ds(pl.multiple_of(j * HD, HD), HD)] = out.astype(jnp.bfloat16)

    def mix_pair(i, c):
        mix(2 * i)
        mix(2 * i + 1)
        return c

    lax.fori_loop(0, heads // 2, mix_pair, 0)
    stores[2].start()
    for kind in range(3):
        settle(held[kind], send_sem.at[kind])
        settle(outgoing[kind], send_sem.at[3 + kind])
    for store in stores:
        store.wait()


def solution(mesh):
    n = mesh.shape["req"]

    def local(
        cache_states,
        pool_keys,
        pool_values,
        slot_prefix,
        page_table,
        prefix_id,
        lengths,
        queries,
        suffix_keys,
        suffix_values,
        u_in,
        dt_raw,
        bc_in,
        a_log,
        dt_bias,
        d_skip,
    ):
        nstate, channels = a_log.shape
        tokens = u_in.shape[0]
        kv = suffix_keys.shape[1]
        prefix_len = pool_keys.shape[0] * pool_keys.shape[1]
        heads = queries.shape[1] // HD
        page = pool_keys.shape[1]
        size = min(page, prefix_len // n)
        chunks = prefix_len // size
        per = chunks // n
        me = lax.axis_index("req")
        slots = jnp.arange(n, dtype=jnp.int32)
        source = jnp.sum(jnp.where(slot_prefix[None] == prefix_id[:, None], slots[None], 0), axis=1)
        pages = page_table[prefix_id[me]]
        inner = jnp.arange(page // size, dtype=jnp.int32)
        chunk_order = (pages[:, None] * (page // size) + inner[None]).reshape(-1)
        width = channels // n
        blocks = channels // WIDE
        bf, f32 = jnp.bfloat16, jnp.float32
        smem = pl.BlockSpec(memory_space=pltpu.SMEM)
        vmem = pl.BlockSpec(memory_space=pltpu.VMEM)
        hbm = pl.BlockSpec(memory_space=pl.ANY)
        total = prefix_len + tokens
        scratch = (
            ([pltpu.VMEM((n, nstate, width), bf)] + [pltpu.VMEM((n, per, size, kv), bf)] * 2) * 2
            + [pltpu.VMEM((n, nstate, width), bf)] + [pltpu.VMEM((chunks, size, kv), bf)] * 2
            + [
                pltpu.VMEM((total, kv), bf),
                pltpu.VMEM((total, kv), bf),
                pltpu.VMEM(queries.shape, bf),
                pltpu.VMEM(u_in.shape, bf),
                pltpu.VMEM(dt_raw.shape, bf),
                pltpu.VMEM(a_log.shape, f32),
                pltpu.VMEM(u_in.shape, bf),
                pltpu.VMEM(queries.shape, bf),
                pltpu.VMEM(a_log.shape, f32),
                pltpu.VMEM((blocks, tokens * SUB, LANE), f32),
                pltpu.VMEM((blocks, tokens * SUB, LANE), f32),
                pltpu.VMEM((tokens * SUB, LANE), f32),
                pltpu.VMEM((nstate * SUB, LANE), f32),
                pltpu.VMEM((blocks, nstate * SUB, LANE), f32),
                pltpu.VMEM((2 * nstate, tokens * SUB, LANE), f32),
                pltpu.VMEM((heads, tokens, total), bf),
                pltpu.VMEM((heads, tokens, HD), f32),
                pltpu.SemaphoreType.DMA((6,)),
                pltpu.SemaphoreType.DMA((6,)),
                pltpu.SemaphoreType.DMA((3,)),
                pltpu.SemaphoreType.DMA((6,)),
                pltpu.SemaphoreType.DMA((3,)),
            ]
        )
        mamba, attn, final = pl.pallas_call(
            functools.partial(kernel, n),
            out_shape=(
                jax.ShapeDtypeStruct(u_in.shape, bf),
                jax.ShapeDtypeStruct(queries.shape, bf),
                jax.ShapeDtypeStruct(a_log.shape, f32),
            ),
            in_specs=[smem] * 3 + [vmem] * 3 + [hbm] * 9,
            out_specs=(hbm, hbm, hbm),
            scratch_shapes=scratch,
            compiler_params=pltpu.CompilerParams(
                collective_id=0, has_side_effects=True, vmem_limit_bytes=64 * 1000 * 1024
            ),
        )(
            source,
            chunk_order,
            lengths,
            bc_in[0][:, :, None],
            dt_bias[None],
            d_skip[None],
            cache_states[0],
            pool_keys.reshape(chunks, size, kv),
            pool_values.reshape(chunks, size, kv),
            queries,
            suffix_keys,
            suffix_values,
            u_in,
            dt_raw,
            a_log,
        )
        return mamba, attn, final[None]

    split = ("groups", "req")
    one, two, three = P(split), P(split, None), P(split, None, None)
    return jax.shard_map(
        local,
        mesh=mesh,
        in_specs=(
            three,
            three,
            three,
            P("groups"),
            P("groups", None),
            P("groups"),
            one,
            two,
            two,
            two,
            two,
            two,
            three,
            P(),
            P(),
            P(),
        ),
        out_specs=(two, two, three),
        check_vma=False,
    )
```

```python
import functools
import math

import jax
import jax.numpy as jnp
from jax import lax
from jax.experimental import pallas as pl
from jax.experimental.pallas import tpu as pltpu
from jax.sharding import PartitionSpec as P

HD = 128
MESH = pl.DeviceIdType.MESH
LOG2E = 1.4426950408889634
SUB = 8
LANE = 128
WIDE = SUB * LANE
CAPS = (3, 4, 5)


def plan_kernel(
    n, w, slot_prefix, prefix_id, page_table, where_ref, source, order, right, left, final, need, far_r, far_l, before
):
    me = where_ref[0]
    p = me // w
    planes = n // w

    def clear(s, c):
        far_r[s] = -1
        far_l[s] = n
        return c

    lax.fori_loop(0, n, clear, 0)

    def invert(s, c):
        before[slot_prefix[s]] = s
        return c

    lax.fori_loop(0, n, invert, 0)

    def find(r, c):
        s = before[prefix_id[r]]
        source[r] = s
        far_r[s] = jnp.maximum(far_r[s], r // w)
        far_l[s] = jnp.minimum(far_l[s], r // w)
        return c

    lax.fori_loop(0, n, find, 0)

    def pages(k, c):
        order[k] = page_table[prefix_id[me], k]
        return c

    lax.fori_loop(0, page_table.shape[1], pages, 0)

    def start(k, c):
        for ref in (right, left):
            ref[0, k] = 0
            ref[1, k] = -1
        return c

    lax.fori_loop(0, n, start, 0)

    def fill(k, c):
        own = source[p * w + k] - p * w
        inside = (own >= 0) & (own < w)
        final[0, k] = jnp.where(inside, own, 0)
        final[1, k] = -1
        return c

    lax.fori_loop(0, w, fill, 0)

    def listing(cut, going_right, worst):
        into = right if going_right else left
        arriving = (p == cut + 1) if going_right else (p == cut)
        leaving = (p == cut) if going_right else (p == cut + 1)

        def by_distance(e, count):
            reach = planes - 1 - e if going_right else e

            def add(s, count):
                at = s // w
                if going_right:
                    hit = (at <= cut) & (far_r[s] == reach) & (reach > cut)
                else:
                    hit = (at > cut) & (far_l[s] == reach) & (reach <= cut)

                @pl.when(hit & leaving)
                def _():
                    relayed = at != p
                    into[0, count] = jnp.where(relayed, 0, s - p * w)
                    into[1, count] = jnp.where(relayed, before[s], -1)

                @pl.when(hit & arriving)
                def _():
                    before[s] = count

                    def serve(k, c):
                        @pl.when(source[p * w + k] == s)
                        def _():
                            final[1, k] = 2 * count + (0 if going_right else 1)

                        return c

                    lax.fori_loop(0, w, serve, 0)

                return count + jnp.where(hit, 1, 0)

            return lax.fori_loop(0, n, add, count)

        steps = planes - 1
        count = lax.fori_loop(0, steps, by_distance, jnp.int32(0))
        return jnp.maximum(worst, count)

    worst = lax.fori_loop(0, planes - 1, lambda c, m: listing(c, True, m), jnp.int32(0))
    worst = lax.fori_loop(0, planes - 1, lambda c, m: listing(planes - 2 - c, False, m), worst)
    need[0] = worst


def kernel(n, w, cap, *refs):
    (source, order, right, left, final, lengths, bc_cols, dt_bias, d_skip) = refs[:9]
    (cache, pool_k, pool_v, q_hbm, sk_hbm, sv_hbm, u_hbm, dt_hbm, a_hbm) = refs[9:18]
    (mamba_hbm, attn_hbm, final_hbm) = refs[18:21]
    (held_s, held_k, held_v, send_s, send_k, send_v, got_s, got_k, got_v) = refs[21:30]
    (keys, values, q_v, u_v, dt_v, a_v, mamba_v, attn_v, final_v) = refs[30:39]
    (delta_w, du_w, y_w, h_w, rate_w, bc_w, w_w, inv_w) = refs[39:47]
    (send_sem, recv_sem, own_sem, in_sem, out_sem) = refs[47:52]
    if cap:
        (hop_send, hop_recv) = refs[52:54]
        boxes = refs[54:]
    me = lax.axis_index("req")
    p = lax.div(me, w)
    mine = lax.rem(me, w)
    planes = n // w
    tokens, channels = u_v.shape
    nstate = a_v.shape[0]
    blocks = channels // WIDE
    width = held_s.shape[2]
    total = keys.shape[0]
    prefix_len = total - tokens
    chunks, size, _ = got_k.shape
    per = chunks // w
    heads = q_v.shape[1] // HD
    q_group = heads // (keys.shape[1] // HD)

    def box(kind, outward, way, k):
        return boxes[((kind * 2 + outward) * 2 + way) * cap + k]

    loads = [
        pltpu.make_async_copy(dt_hbm, dt_v, in_sem.at[0]),
        pltpu.make_async_copy(u_hbm, u_v, in_sem.at[1]),
        pltpu.make_async_copy(a_hbm, a_v, in_sem.at[2]),
        pltpu.make_async_copy(q_hbm, q_v, in_sem.at[3]),
        pltpu.make_async_copy(sk_hbm, keys.at[pl.ds(prefix_len, tokens)], in_sem.at[4]),
        pltpu.make_async_copy(sv_hbm, values.at[pl.ds(prefix_len, tokens)], in_sem.at[5]),
    ]
    for load in loads:
        load.start()

    barrier = pltpu.get_barrier_semaphore()
    sides = (p < planes - 1, p > 0)

    def greet(peer):
        pl.semaphore_signal(barrier, inc=1, device_id={"req": peer}, device_id_type=MESH)

    def greet_step(d, c):
        greet(p * w + lax.rem(mine + d, w))
        return c

    lax.fori_loop(1, w, greet_step, 0)
    for way in range(2 if cap else 0):

        @pl.when(jnp.logical_not(sides[1 - way]))
        def _():
            for kind in range(3):
                for k in range(cap):
                    ref = box(kind, 0, way, k)
                    ref[...] = jnp.zeros_like(ref)

        @pl.when(sides[way])
        def _():
            greet(me + w if way == 0 else me - w)

    near = sides[0].astype(jnp.int32) + sides[1].astype(jnp.int32) if cap else 0
    pl.semaphore_wait(barrier, w - 1 + near)

    def part(kind, index):
        if kind == 0:
            return cache.at[:, pl.ds(pl.multiple_of(index * width, width), width)]
        pool = pool_k if kind == 1 else pool_v
        return pool.at[pl.ds(index * per, per)]

    held = (held_s, held_k, held_v)
    outgoing = (send_s, send_k, send_v)
    got = (got_s, got_k, got_v)

    def spread(kind):
        own = pltpu.make_async_copy(part(kind, mine), held[kind].at[mine], own_sem.at[kind])
        own.start()

        def step(d, c):
            other = lax.rem(mine + d, w)
            pltpu.make_async_remote_copy(
                src_ref=part(kind, other),
                dst_ref=held[kind].at[mine],
                send_sem=send_sem.at[kind],
                recv_sem=recv_sem.at[kind],
                device_id={"req": p * w + other},
                device_id_type=MESH,
            ).start()
            return c

        lax.fori_loop(1, w, step, 0)

    def settle(ref, sem):
        piece = ref.at[pl.ds(0, ref.shape[0] // w * (w - 1))]
        pltpu.make_async_copy(piece, piece, sem).wait()

    def gathered(kind):
        settle(held[kind], recv_sem.at[kind])
        pltpu.make_async_copy(part(kind, mine), held[kind].at[mine], own_sem.at[kind]).wait()

    def crossing(kind, way, k):
        return pltpu.make_async_remote_copy(
            src_ref=box(kind, 1, way, k),
            dst_ref=box(kind, 0, way, k),
            send_sem=hop_send.at[(kind * 2 + way) * cap + k],
            recv_sem=hop_recv.at[(kind * 2 + way) * cap + k],
            device_id={"req": me + w if way == 0 else me - w},
            device_id_type=MESH,
        )

    def hop(kind, k):
        for way in range(2):
            table = (right, left)[way]

            @pl.when(sides[1 - way])
            def _():
                crossing(kind, way, k).wait_recv()

            @pl.when(sides[way])
            def _():
                item = held[kind][table[0, k]]
                code = table[1, k]
                for e in range(k + 1):
                    item = jnp.where(code == e, box(kind, 0, way, e)[...], item)
                box(kind, 1, way, k)[...] = item
                crossing(kind, way, k).start()

    def deliver(kind):
        def choose(r):
            item = held[kind][final[0, r]]
            code = final[1, r]
            for e in range(cap):
                for way in range(2):
                    item = jnp.where(code == 2 * e + way, box(kind, 0, way, e)[...], item)
            return item

        def pick(r, c):
            outgoing[kind][r] = choose(r)
            return c

        lax.fori_loop(0, w, pick, 0)
        if kind == 0:
            landing = got_s.at[mine]
            got_s[mine] = choose(mine)
        else:
            landing = got[kind].at[pl.ds(mine * per, per)]
            got[kind][pl.ds(mine * per, per)] = choose(mine)

        def step(d, c):
            other = lax.rem(mine + d, w)
            pltpu.make_async_remote_copy(
                src_ref=outgoing[kind].at[other],
                dst_ref=landing,
                send_sem=send_sem.at[3 + kind],
                recv_sem=recv_sem.at[3 + kind],
                device_id={"req": p * w + other},
                device_id_type=MESH,
            ).start()
            return c

        lax.fori_loop(1, w, step, 0)

    spread(0)
    spread(1)
    if cap:
        spread(2)

    def widen(k, c):
        bc_w[k] = jnp.broadcast_to(bc_cols[k], (tokens, LANE))
        return c

    lax.fori_loop(0, 2 * nstate, widen, 0)

    length = lengths[0]
    live = lax.broadcasted_iota(jnp.int32, (tokens, LANE), 0) < length
    loads[0].wait()
    loads[1].wait()

    def steps_of(b, c):
        for s in range(SUB):
            at = pl.ds(pl.multiple_of(b * WIDE + s * LANE, LANE), LANE)
            raw = dt_v[:, at].astype(jnp.float32) + dt_bias[:, at]
            soft = jnp.maximum(raw, 0.0) + jnp.log1p(jnp.exp(-jnp.abs(raw)))
            delta = jnp.where(live, soft, 0.0)
            delta_w[b, pl.ds(s, tokens, stride=SUB), :] = delta
            du_w[b, pl.ds(s, tokens, stride=SUB), :] = delta * u_v[:, at].astype(jnp.float32)
        return c

    lax.fori_loop(0, blocks, steps_of, 0)
    gathered(0)
    for k in range(cap):
        hop(0, k)
    deliver(0)
    if not cap:
        spread(2)
    loads[2].wait()

    def rates_of(b, c):
        for s in range(SUB):
            at = pl.ds(pl.multiple_of(b * WIDE + s * LANE, LANE), LANE)
            rate_w[b, pl.ds(s, nstate, stride=SUB), :] = -LOG2E * jnp.exp(a_v[:, at])
        return c

    lax.fori_loop(0, blocks, rates_of, 0)
    gathered(1)
    later = [functools.partial(hop, 1, k) for k in range(cap)] + [functools.partial(deliver, 1)]
    later += [functools.partial(gathered, 2)] + [functools.partial(hop, 2, k) for k in range(cap)]
    later += [functools.partial(deliver, 2)]
    if cap:
        later.pop(0)()
    else:
        later.pop(0)()
    settle(got_s, recv_sem.at[3])

    def scan_block(b, c):
        for s in range(SUB):
            first = b * WIDE + s * LANE
            inside = lax.rem(first, width)
            start = got_s[lax.div(first, width), :, pl.ds(pl.multiple_of(inside, LANE), LANE)]
            h_w[pl.ds(s, nstate, stride=SUB), :] = start.astype(jnp.float32)
        rates = [rate_w[b, pl.ds(k * SUB, SUB), :] for k in range(nstate)]

        def advance(t, hs):
            at = pl.ds(pl.multiple_of(t * SUB, SUB), SUB)
            delta = delta_w[b, at, :]
            du = du_w[b, at, :]
            new = []
            sums = [None, None]
            for k in range(nstate):
                h = jnp.exp2(delta * rates[k]) * hs[k] + du * bc_w[k, pl.ds(t, 1), :]
                term = bc_w[nstate + k, pl.ds(t, 1), :] * h
                sums[k % 2] = term if sums[k % 2] is None else sums[k % 2] + term
                new.append(h)
            y_w[at, :] = sums[0] + sums[1]
            return tuple(new)

        def pair(i, hs):
            return advance(2 * i + 1, advance(2 * i, hs))

        hs = tuple(h_w[pl.ds(k * SUB, SUB), :] for k in range(nstate))
        hs = lax.fori_loop(0, tokens // 2, pair, hs)
        for k in range(nstate):
            h_w[pl.ds(k * SUB, SUB), :] = hs[k]
        for s in range(SUB):
            at = pl.ds(pl.multiple_of(b * WIDE + s * LANE, LANE), LANE)
            final_v[:, at] = h_w[pl.ds(s, nstate, stride=SUB), :]
            y = y_w[pl.ds(s, tokens, stride=SUB), :] + d_skip[:, at] * u_v[:, at].astype(jnp.float32)
            mamba_v[:, at] = jnp.where(live, y, 0.0).astype(jnp.bfloat16)
        return c

    at_once = 1 if cap else 4
    for first in range(0, blocks, at_once):
        lax.fori_loop(first, min(first + at_once, blocks), scan_block, 0)
        if later and first + at_once < blocks:
            later.pop(0)()
            if later and later[0].func is gathered:
                later.pop(0)()
    if not cap:
        for job in later:
            job()
        later = []

    stores = [
        pltpu.make_async_copy(mamba_v, mamba_hbm, out_sem.at[0]),
        pltpu.make_async_copy(final_v, final_hbm, out_sem.at[1]),
        pltpu.make_async_copy(attn_v, attn_hbm, out_sem.at[2]),
    ]
    stores[0].start()
    stores[1].start()

    def arrange(kind, into):
        def step(k, c):
            to = pl.ds(pl.multiple_of(k * size, size), size)
            into[to, :] = got[kind][order[lax.div(k, fine)] * fine + lax.rem(k, fine)]
            return c

        fine = chunks // order.shape[0]
        lax.fori_loop(0, chunks, step, 0)

    loads[3].wait()
    loads[4].wait()
    while later and not (later[0].func is hop and later[0].args[0] == 2):
        later.pop(0)()
    settle(got_k, recv_sem.at[4])
    arrange(1, keys)
    factor = LOG2E / math.sqrt(HD)
    row = lax.broadcasted_iota(jnp.int32, (tokens, tokens), 0)
    col = lax.broadcasted_iota(jnp.int32, (tokens, tokens), 1)

    def weigh(j):
        g = lax.div(j, q_group)
        q = q_v[:, pl.ds(pl.multiple_of(j * HD, HD), HD)]
        k = keys[:, pl.ds(pl.multiple_of(g * HD, HD), HD)]
        scores = lax.dot_general(q, k, (((1,), (1,)), ((), ())), preferred_element_type=jnp.float32)
        scores = jnp.concatenate(
            [
                jnp.where(col > row, scores[:, :tokens], -1e30),
                scores[:, tokens:prefix_len],
                jnp.where(col <= row, scores[:, prefix_len:], -1e30),
            ],
            axis=1,
        )
        highest = jnp.max(scores, axis=1, keepdims=True)
        weight = jnp.exp2((scores - highest) * factor)
        inv_w[j] = jnp.broadcast_to(1.0 / jnp.sum(weight, axis=1, keepdims=True), (tokens, HD))
        w_w[j] = weight.astype(jnp.bfloat16)

    def weigh_pair(i, c):
        weigh(2 * i)
        weigh(2 * i + 1)
        return c

    lots = len(later)
    bounds = [heads // 2 * e // (lots + 1) for e in range(lots + 2)]
    for first, last in zip(bounds, bounds[1:]):
        lax.fori_loop(first, last, weigh_pair, 0)
        if later:
            later.pop(0)()
    while later:
        later.pop(0)()

    loads[5].wait()
    settle(got_v, recv_sem.at[5])
    arrange(2, values)

    def mix(j):
        g = lax.div(j, q_group)
        v = values[:, pl.ds(pl.multiple_of(g * HD, HD), HD)]
        out = jnp.dot(w_w[j], v, preferred_element_type=jnp.float32) * inv_w[j]
        out = jnp.where(live, out, 0.0)
        attn_v[:, pl.ds(pl.multiple_of(j * HD, HD), HD)] = out.astype(jnp.bfloat16)

    def mix_pair(i, c):
        mix(2 * i)
        mix(2 * i + 1)
        return c

    lax.fori_loop(0, heads // 2, mix_pair, 0)
    stores[2].start()
    for kind in range(3):
        settle(held[kind], send_sem.at[kind])
        settle(outgoing[kind], send_sem.at[3 + kind])
        for k in range(cap):
            for way in range(2):

                @pl.when(sides[way])
                def _():
                    crossing(kind, way, k).wait_send()

    for store in stores:
        store.wait()


def solution(mesh):
    n, groups = mesh.shape["req"], mesh.shape["groups"]

    def local(
        cache_states,
        pool_keys,
        pool_values,
        slot_prefix,
        page_table,
        prefix_id,
        lengths,
        queries,
        suffix_keys,
        suffix_values,
        u_in,
        dt_raw,
        bc_in,
        a_log,
        dt_bias,
        d_skip,
    ):
        nstate, channels = a_log.shape
        tokens = u_in.shape[0]
        kv = suffix_keys.shape[1]
        prefix_len = pool_keys.shape[0] * pool_keys.shape[1]
        heads = queries.shape[1] // HD
        blocks = channels // WIDE
        bf, f32 = jnp.bfloat16, jnp.float32
        smem = pl.BlockSpec(memory_space=pltpu.SMEM)
        vmem = pl.BlockSpec(memory_space=pltpu.VMEM)
        hbm = pl.BlockSpec(memory_space=pl.ANY)
        total = prefix_len + tokens
        page_count, page = pool_keys.shape[:2]
        plane = 1
        while plane * plane * 4 <= n:
            plane *= 2
        plane = plane if n % plane == 0 else n
        plane = min(plane, n)

        def ints(*shape):
            return jax.ShapeDtypeStruct(shape, jnp.int32)

        me = lax.axis_index("req").astype(jnp.int32).reshape(1)
        source, order, right, left, final_plan, need = pl.pallas_call(
            functools.partial(plan_kernel, n, plane),
            out_shape=(ints(n), ints(page_count), ints(2, n), ints(2, n), ints(2, n), ints(1)),
            in_specs=[smem] * 4,
            out_specs=(smem,) * 6,
            scratch_shapes=[pltpu.SMEM((n,), jnp.int32)] * 3,
        )(slot_prefix, prefix_id, page_table, me)
        shift = 1
        while shift < groups:
            ring = [(g, (g + shift) % groups) for g in range(groups)]
            need = jnp.maximum(need, lax.ppermute(need, "groups", ring))
            shift *= 2

        def build(w, cap, number):
            size = min(page, prefix_len // w)
            chunks = prefix_len // size
            per = chunks // w
            width = channels // w
            state = (nstate, width)
            piece = (per, size, kv)
            item = [pltpu.VMEM(state, bf)] * (4 * cap) + [pltpu.VMEM(piece, bf)] * (8 * cap)
            hops = [pltpu.SemaphoreType.DMA((6 * cap,))] * 2 + item if cap else []
            scratch = (
                ([pltpu.VMEM((w, *state), bf)] + [pltpu.VMEM((w, *piece), bf)] * 2) * 2
                + [pltpu.VMEM((w, *state), bf)]
                + [pltpu.VMEM((chunks, size, kv), bf)] * 2
                + [
                    pltpu.VMEM((total, kv), bf),
                    pltpu.VMEM((total, kv), bf),
                    pltpu.VMEM(queries.shape, bf),
                    pltpu.VMEM(u_in.shape, bf),
                    pltpu.VMEM(dt_raw.shape, bf),
                    pltpu.VMEM(a_log.shape, f32),
                    pltpu.VMEM(u_in.shape, bf),
                    pltpu.VMEM(queries.shape, bf),
                    pltpu.VMEM(a_log.shape, f32),
                    pltpu.VMEM((blocks, tokens * SUB, LANE), f32),
                    pltpu.VMEM((blocks, tokens * SUB, LANE), f32),
                    pltpu.VMEM((tokens * SUB, LANE), f32),
                    pltpu.VMEM((nstate * SUB, LANE), f32),
                    pltpu.VMEM((blocks, nstate * SUB, LANE), f32),
                    pltpu.VMEM((2 * nstate, tokens, LANE), f32),
                    pltpu.VMEM((heads, tokens, total), bf),
                    pltpu.VMEM((heads, tokens, HD), f32),
                    pltpu.SemaphoreType.DMA((6,)),
                    pltpu.SemaphoreType.DMA((6,)),
                    pltpu.SemaphoreType.DMA((3,)),
                    pltpu.SemaphoreType.DMA((6,)),
                    pltpu.SemaphoreType.DMA((3,)),
                ]
                + hops
            )

            def run(*args):
                (source, final_plan, order, right, left, pool_keys, pool_values, *rest) = args
                final_plan = final_plan if cap else jnp.stack([source, jnp.full_like(source, -1)])
                pools = (pool_keys.reshape(chunks, size, kv), pool_values.reshape(chunks, size, kv))
                return pl.pallas_call(
                    functools.partial(kernel, n, w, cap),
                    out_shape=(
                        jax.ShapeDtypeStruct(u_in.shape, bf),
                        jax.ShapeDtypeStruct(queries.shape, bf),
                        jax.ShapeDtypeStruct(a_log.shape, f32),
                    ),
                    in_specs=[smem] * 6 + [vmem] * 3 + [hbm] * 9,
                    out_specs=(hbm, hbm, hbm),
                    scratch_shapes=scratch,
                    compiler_params=pltpu.CompilerParams(
                        collective_id=number, has_side_effects=True, vmem_limit_bytes=64 * 1000 * 1024
                    ),
                )(source, order, right, left, final_plan, *rest[:5], *pools, *rest[5:])

            return run

        args = (
            source,
            final_plan,
            order,
            right,
            left,
            pool_keys,
            pool_values,
            lengths,
            bc_in[0][:, :, None],
            dt_bias[None],
            d_skip[None],
            cache_states[0],
            queries,
            suffix_keys,
            suffix_values,
            u_in,
            dt_raw,
            a_log,
        )
        caps = CAPS
        choices = [build(plane, cap, e) for e, cap in enumerate(caps)] + [build(n, 0, len(caps))]
        which = sum((need[0] > cap).astype(jnp.int32) for cap in caps)
        mamba, attn, final = lax.switch(which, choices, *args)
        return mamba, attn, final[None]

    split = ("groups", "req")
    one, two, three = P(split), P(split, None), P(split, None, None)
    return jax.shard_map(
        local,
        mesh=mesh,
        in_specs=(
            three,
            three,
            three,
            P("groups"),
            P("groups", None),
            P("groups"),
            one,
            two,
            two,
            two,
            two,
            two,
            three,
            P(),
            P(),
            P(),
        ),
        out_specs=(two, two, three),
        check_vma=False,
    )
```
